32 devices in a mesh: mesh: 8 (over z, y), member: 4 (over x, core).
Axes of the slice: x: 2, y: 2, z: 4, core: 2. Of those that a mesh axis runs over, the one named last changes fastest.
Arguments:
- node_states: bfloat16 [8, 4096, 512], P('member', 'mesh'), may hold values from -60 to 60
- projection: bfloat16 [512, 1536], P('member'), may hold values from -12 to 12
- output_weight: bfloat16 [512, 512], P('member'), may hold values from -0.25 to 0.25
- up_weight: bfloat16 [512, 2048], P('member'), may hold values from -0.25 to 0.25
- down_weight: bfloat16 [2048, 512], P('member'), may hold values from -0.125 to 0.125
- attention_gain: float32 [512], replicated, may hold values from 0.5 to 2
- feedforward_gain: float32 [512], replicated, may hold values from 0.5 to 2
- tile_lists: int32 [32, 8], P('mesh'), may hold values from 0 to 31, as said below
- tile_counts: int32 [32], P('mesh'), may hold values from 4 to 8, as said below
Outputs:
- updated_states: bfloat16 [8, 4096, 512], P('member', 'mesh')
The draws below stay inside these ranges and needn't reach their ends.
Inputs may be any that keep to these rules, and one draw needn't show every extreme that they name: `tile_lists`: entry 0 of tile t's list is t. Every entry names a tile of the device that holds t, or one of the last 4 tiles of the device before it, or one of the first 4 tiles of the device after it along mesh (the first and last devices are neighbours). The first tile_counts[t] entries are distinct; later entries are ignored. `tile_counts`: every device holds a tile whose count is 8.
All inputs are finite; a program needn't handle non-finite values.
Results may differ from the reference program's by a relative error of at most 0.0056.
Values may be sent and summed in bfloat16 or wider, within the bound.
A program may use at most 128 MiB of HBM per device.

```python
import math
import jax
import jax.numpy as jnp
from jax import lax

D = 512
HEADS = 4
FF = 2048
TILE = 128
TILES_DEV = 4
RIM_T = 4
KT = 8
MEMBERS = 8
TILES = 32
NODES = 4096


def draw_node_states(key, part):
    sample = jax.random.normal(key, (MEMBERS, NODES, D), jnp.float32)
    return jnp.clip(sample, -60.0, 60.0).astype(jnp.bfloat16)


def draw_projection(key, part):
    sample = jnp.clip(jax.random.normal(key, (D, 3 * D), jnp.float32), -6.0, 6.0) * D ** (-0.5)
    return jnp.clip(sample, -12.0, 12.0).astype(jnp.bfloat16)


def tile_plan(key):
    sample = jax.random.fold_in(key, 7)
    devices = TILES // TILES_DEV
    window_tiles = TILES_DEV + 2 * RIM_T
    tile_ids = jnp.arange(TILES, dtype=jnp.int32)
    owner = tile_ids // TILES_DEV
    inner = tile_ids % TILES_DEV
    tile_keys = jax.random.split(sample, TILES)

    def pick(tile_key, own):
        shuffled = jax.random.permutation(tile_key, window_tiles - 1).astype(jnp.int32)
        shuffled = jnp.where(shuffled >= own, shuffled + 1, shuffled)
        return jnp.concatenate([own[None], shuffled[:KT - 1]])
    entries = jax.vmap(pick)(tile_keys, inner + RIM_T)
    owner_col = owner[:, None]
    leading = jnp.mod(owner_col - 1, devices) * TILES_DEV + TILES_DEV - RIM_T + entries
    middle = owner_col * TILES_DEV + entries - RIM_T
    trailing = jnp.mod(owner_col + 1, devices) * TILES_DEV + entries - RIM_T - TILES_DEV
    global_ids = jnp.where(entries < RIM_T, leading, jnp.where(entries < RIM_T + TILES_DEV, middle, trailing))
    counts = jax.random.randint(jax.random.fold_in(sample, 1), (TILES,), (KT + 1) // 2, KT + 1).astype(jnp.int32)
    counts = jnp.where(inner == 0, KT, counts).astype(jnp.int32)
    column = jnp.arange(KT, dtype=jnp.int32)
    global_ids = jnp.where(column[None, :] < counts[:, None], global_ids, tile_ids[:, None])
    return (global_ids.astype(jnp.int32), counts)


def draw_tile_lists(key, part):
    return tile_plan(key)[0]


def draw_tile_counts(key, part):
    return tile_plan(key)[1]


def steps_of(own_key, shape, cuts, low, largest):
    level, own = 1.0, jax.random.fold_in(own_key, 6)
    for axis_at, blocks in cuts:
        steps = jnp.exp(jax.random.uniform(jax.random.fold_in(own, axis_at), (blocks,), jnp.float32, low / len(cuts), largest / len(cuts)))
        level = level * jnp.repeat(steps, shape[axis_at] // blocks).reshape([-1 if axis == axis_at else 1 for axis in range(len(shape))])
    return level


def normal_values(rng, shape, scale, reach, pieces=(), kind=jnp.bfloat16):
    loudness = steps_of(rng, shape, pieces, -0.22, 0.18) if pieces else 1.0
    result = jax.random.normal(rng, shape, jnp.float32) * scale * loudness
    return jnp.minimum(jnp.maximum(result, -reach), reach).astype(kind)


def setup_inputs(seed: int = 0) -> dict:
    key_list = jax.random.split(jax.random.key(seed), 10)
    return {
        "node_states": draw_node_states(jax.random.fold_in(key_list[9], 71), 0),
        "projection": draw_projection(jax.random.fold_in(key_list[9], 71), 0),
        "output_weight": normal_values(key_list[2], (D, D), D ** -0.5, 0.25, ((0, 4),)),
        "up_weight": normal_values(key_list[3], (D, FF), D ** -0.5, 0.25, ((0, 4),)),
        "down_weight": normal_values(key_list[4], (FF, D), FF ** -0.5, 0.125, ((0, 4),)),
        "attention_gain": jnp.clip(jnp.exp(jax.random.uniform(key_list[5], (D,), jnp.float32, math.log(0.5), math.log(2.0))), 0.5, 2.0),
        "feedforward_gain": jnp.clip(jnp.exp(jax.random.uniform(key_list[6], (D,), jnp.float32, math.log(0.5), math.log(2.0))), 0.5, 2.0),
        "tile_lists": draw_tile_lists(jax.random.fold_in(key_list[9], 71), 0),
        "tile_counts": draw_tile_counts(jax.random.fold_in(key_list[9], 71), 0),
    }


def layer_norm(node_rows, gain):
    values = node_rows.astype(jnp.float32)
    center = values - lax.optimization_barrier(jnp.mean(values, axis=-1, keepdims=True))
    spread = lax.optimization_barrier(jnp.mean(center * center, axis=-1, keepdims=True))
    return (center * lax.rsqrt(spread + 1e-05) * gain).astype(jnp.bfloat16)

def attend(queries, window, tile_ids, counts):
    members, groups, tile_rows, model_width = queries.shape
    entries = tile_ids.shape[1]
    head_size = model_width // HEADS
    picked = jnp.take(window, tile_ids.reshape(-1), axis=1)
    picked = picked.reshape(members, groups, entries * tile_rows, 2 * model_width)
    key_part = picked[..., :model_width].reshape(members, groups, entries * tile_rows, HEADS, head_size).astype(jnp.float32)
    value_part = picked[..., model_width:].reshape(members, groups, entries * tile_rows, HEADS, head_size).astype(jnp.float32)
    query_part = queries.reshape(members, groups, tile_rows, HEADS, head_size).astype(jnp.float32)
    scores = jnp.einsum('mgqhe,mgkhe->mghqk', query_part, key_part) / math.sqrt(head_size)
    usable = (jnp.arange(entries * tile_rows) // tile_rows)[None, :] < counts[:, None]
    scores = jnp.where(usable[None, :, None, None, :], scores, -jnp.inf)
    highest = lax.optimization_barrier(jnp.max(scores, axis=-1, keepdims=True))
    weights = jnp.exp(scores - highest)
    summed = lax.optimization_barrier(jnp.sum(weights, axis=-1, keepdims=True))
    rounded = lax.optimization_barrier(weights.astype(jnp.bfloat16)).astype(jnp.float32)
    blended = jnp.einsum('mghqk,mgkhe->mghqe', rounded, value_part) / summed
    blended = jnp.transpose(blended, (0, 1, 3, 2, 4)).reshape(members, groups, tile_rows, model_width)
    return blended.astype(jnp.bfloat16)

def reference(node_states, projection, output_weight, up_weight, down_weight, attention_gain, feedforward_gain, tile_lists, tile_counts):
    members, node_count, model_width = node_states.shape
    normed = layer_norm(node_states, attention_gain)

    def project(node_rows):
        projected = jnp.dot(node_rows, projection, preferred_element_type=jnp.float32)
        return (projected[:, :model_width].astype(jnp.bfloat16), projected[:, model_width:].astype(jnp.bfloat16))
    queries, pairs = lax.map(project, normed)
    window = pairs.reshape(members, TILES, TILE, 2 * model_width)
    grouped = jnp.transpose(queries.reshape(members, TILES // 2, 2, TILE, model_width), (1, 0, 2, 3, 4))
    lists_grouped = tile_lists.reshape(TILES // 2, 2, KT)
    counts_grouped = tile_counts.reshape(TILES // 2, 2)

    def one_group(element):
        return attend(element[0], window, element[1], element[2])
    attended = lax.map(one_group, (grouped, lists_grouped, counts_grouped))
    attended = jnp.transpose(attended, (1, 0, 2, 3, 4)).reshape(members, node_count, model_width)

    def finish(element):
        states, blended = element
        middle = (states.astype(jnp.float32) + jnp.dot(blended, output_weight, preferred_element_type=jnp.float32)).astype(jnp.bfloat16)
        middle = lax.optimization_barrier(middle)
        normed_second = layer_norm(middle, feedforward_gain)
        hidden = jax.nn.gelu(jnp.dot(normed_second, up_weight, preferred_element_type=jnp.float32), approximate=True).astype(jnp.bfloat16)
        return (middle.astype(jnp.float32) + jnp.dot(hidden, down_weight, preferred_element_type=jnp.float32)).astype(jnp.bfloat16)
    return lax.map(finish, (node_states, attended))
```

```python
import functools
import math

import jax
import jax.numpy as jnp
from jax import lax
from jax.experimental import pallas as pl
from jax.experimental.pallas import tpu as pltpu
from jax.sharding import PartitionSpec as P

HEADS = 4
RIM_T = 4
MESH = pl.DeviceIdType.MESH
MASKED = -1e30
SHARED = -1
EPS = 1e-05


def norm_rows(rows, gain):
    values = rows.astype(jnp.float32)
    center = values - jnp.mean(values, axis=-1, keepdims=True)
    spread = jnp.mean(center * center, axis=-1, keepdims=True)
    return (center * lax.rsqrt(spread + EPS) * gain).astype(jnp.bfloat16)


def gelu(value):
    inner = math.sqrt(2.0 / math.pi) * (value + 0.044715 * value * value * value)
    return 0.5 * value * (1.0 + jnp.tanh(inner))


def dot(a, b):
    return jnp.dot(a, b, preferred_element_type=jnp.float32)


def kernel(
    ring, party, tiles,
    x_hbm, proj_hbm, wo_hbm, up_hbm, down_hbm, gain1_hbm, gain2_hbm, lists_hbm, counts_hbm,
    out_ref,
    xs, wproj, wo, up, down, q_s, k_s, v_s, acc, top, att, hid, mid, bias, gain1, gain2, lists, counts,
    local_sem, xp_send, xp_recv, xf_send, xf_recv, w_send, w_recv,
):
    members, rows, width = x_hbm.shape
    tile = rows // tiles
    head = width // HEADS
    groups = party // 2
    me = lax.axis_index("mesh")
    mine = lax.axis_index("member")
    parity = lax.rem(me, 2)
    side = 1 - 2 * parity
    partner = me + side
    onward = lax.rem(me + 2 * side + ring, ring)
    behind = lax.rem(me - 2 * side + ring, ring)
    core = lax.rem(mine, 2)
    twin = mine + 1 - 2 * core
    across = [lax.rem(mine + 2 * d, party) for d in range(1, groups)]

    barrier = pltpu.get_barrier_semaphore()
    for peer in (partner, onward, behind):
        pl.semaphore_signal(barrier, inc=1, device_id={"mesh": peer}, device_id_type=MESH)
    for peer in [twin] + across:
        pl.semaphore_signal(barrier, inc=1, device_id={"member": peer}, device_id_type=MESH)
    pl.semaphore_wait(barrier, 4 + len(across))

    pieces = [(m, t) for m in range(members) for t in range(tiles)]

    def piece(ref, m, t):
        return ref.at[m, pl.ds(t * tile, tile)]

    to_partner = []
    for i, (m, t) in enumerate(pieces):
        to_partner.append(pltpu.make_async_remote_copy(
            src_ref=piece(x_hbm, m, t), dst_ref=piece(xs.at[1], m, t),
            send_sem=xp_send.at[i], recv_sem=xp_recv.at[i],
            device_id={"mesh": partner}, device_id_type=MESH))
    to_onward = []
    for i, (m, t) in enumerate(pieces):
        to_onward.append(pltpu.make_async_remote_copy(
            src_ref=piece(xs.at[1], m, t), dst_ref=piece(xs.at[2], m, t),
            send_sem=xf_send.at[i], recv_sem=xf_recv.at[i],
            device_id={"mesh": onward}, device_id_type=MESH))

    odd = lax.rem(me // 2, 2)
    aside = me + 2 - 4 * odd
    shards = (proj_hbm, wo_hbm, up_hbm, down_hbm)
    wholes = (wproj, wo, up, down)

    def part(w, who):
        depth = shards[w].shape[0]
        return wholes[w].at[pl.ds(pl.multiple_of(who * depth, depth), depth)]

    lanes = 1 + 4 * (groups - 1)

    def weight_copy(w, lane, src, dst, target):
        return pltpu.make_async_remote_copy(
            src_ref=src, dst_ref=dst,
            send_sem=w_send.at[w * lanes + lane], recv_sem=w_recv.at[w * lanes + lane],
            device_id=target, device_id_type=MESH)

    to_twin, to_across, to_side, near_pass, far_pass = [], [], [], [], []
    for w in range(4):
        to_twin.append(weight_copy(w, 0, shards[w], part(w, mine), {"member": twin}))
        for row in (to_across, to_side, near_pass, far_pass):
            row.append([])
        depth = shards[w].shape[0] // 2

        def half_part(who, which):
            return wholes[w].at[pl.ds(pl.multiple_of((2 * who + which) * depth, depth), depth)]

        for d in range(1, groups):
            giver = lax.rem(mine + party - 2 * d, party)
            lane = 4 * d - 3
            if w == SHARED:
                got, other = half_part(giver, odd), half_part(giver, 1 - odd)
                to_across[w].append(weight_copy(
                    w, lane, shards[w].at[pl.ds(pl.multiple_of(odd * depth, depth), depth)],
                    half_part(mine, odd), {"member": across[d - 1]}))
                to_side[w].append(weight_copy(w, lane + 2, got, got, {"mesh": aside}))
                far_pass[w].append(weight_copy(w, lane + 3, other, other, {"member": twin}))
            else:
                got = part(w, giver)
                to_across[w].append(weight_copy(
                    w, lane, shards[w], part(w, mine), {"member": across[d - 1]}))
            near_pass[w].append(weight_copy(w, lane + 1, got, got, {"member": twin}))

    for copy in to_across[0]:
        copy.start()
    to_partner[0].start()
    to_twin[0].start()
    for copy in to_partner[1:]:
        copy.start()
    for w in range(1, 4):
        for copy in to_across[w]:
            copy.start()
        to_twin[w].start()
    x_local = pltpu.make_async_copy(x_hbm, xs.at[0], local_sem.at[0])
    x_local.start()
    w_local = [pltpu.make_async_copy(shards[w], part(w, mine), local_sem.at[1 + w])
               for w in range(4)]
    for copy in w_local:
        copy.start()
    small = [pltpu.make_async_copy(src, dst, local_sem.at[5 + i]) for i, (src, dst) in enumerate(
        ((gain1_hbm, gain1), (gain2_hbm, gain2), (lists_hbm, lists), (counts_hbm, counts)))]
    for copy in small:
        copy.start()
    v_s[:, :, head:] = jnp.ones((HEADS, rows, head), jnp.bfloat16)
    for copy in small:
        copy.wait()

    def pass_near(w):
        for d in range(groups - 1):
            to_across[w][d].wait_recv()
            if w == SHARED:
                to_side[w][d].start()
            near_pass[w][d].start()

    def pass_far(w):
        for d in range(groups - 1):
            to_side[w][d].wait_recv()
            far_pass[w][d].start()

    def have_weight(w):
        w_local[w].wait()
        to_twin[w].wait_recv()
        for copy in near_pass[w] + far_pass[w]:
            copy.wait_recv()

    def pass_pieces(first, last):
        for i in range(first, last):
            to_partner[i].wait_recv()
            to_onward[i].start()

    every = tiles * ring
    start = me * tiles

    def fill_bias(t, carry):
        count = counts[t]
        places = []
        for j in range(lists.shape[1]):
            place = lists[t, j] - start + RIM_T
            place = jnp.where(place < 0, place + every, place)
            place = jnp.where(place >= every, place - every, place)
            places.append(jnp.where(j < count, place, -1))
        for c in range(3 * tiles):
            if c < tiles:
                want = RIM_T + c
            elif c < 2 * tiles:
                want = jnp.where(parity == 0, RIM_T + tiles + c - tiles, RIM_T - tiles + c - tiles)
            else:
                want = jnp.where(parity == 0, RIM_T - tiles + c - 2 * tiles, RIM_T + tiles + c - 2 * tiles)
            hit = places[0] == want
            for place in places[1:]:
                hit = jnp.logical_or(hit, place == want)
            bias[t, c] = jnp.where(hit, 0.0, MASKED)
        return carry

    lax.fori_loop(0, tiles, fill_bias, 0)

    query_scale = math.log2(math.e) / math.sqrt(head)

    def project(slot, m):
        normed = norm_rows(xs[slot, m], gain1[...].reshape(1, width))
        if slot == 0:
            queries = (dot(normed, wproj[:, :width]) * query_scale).astype(jnp.bfloat16)
            for h in range(HEADS):
                q_s[m, h] = queries[:, h * head:(h + 1) * head]
        keys = dot(normed, wproj[:, width:2 * width]).astype(jnp.bfloat16)
        for h in range(HEADS):
            k_s[h] = keys[:, h * head:(h + 1) * head]
        values = dot(normed, wproj[:, 2 * width:]).astype(jnp.bfloat16)
        for h in range(HEADS):
            v_s[h, :, :head] = values[:, h * head:(h + 1) * head]

    together = 2

    def attend(slot, m):
        marks = [[bias[t, slot * tiles + c] for c in range(tiles)] for t in range(tiles)]

        def body(pair, carry):
            for i in range(together):
                h = pair * together + i
                scores = lax.dot_general(
                    q_s[m, h], k_s[h], (((1,), (1,)), ((), ())),
                    preferred_element_type=jnp.float32)
                packed, fades = [], []
                for t in range(tiles):
                    here = slice(t * tile, (t + 1) * tile)
                    parts = [scores[here, c * tile:(c + 1) * tile] + marks[t][c]
                             for c in range(tiles)]
                    best = parts[0]
                    for p in parts[1:]:
                        best = jnp.maximum(best, p)
                    best = jnp.broadcast_to(jnp.max(best, axis=-1, keepdims=True), (tile, tile))
                    if slot > 0:
                        old = top[m, h, here, :]
                        best = jnp.maximum(best, old)
                        fades.append(jnp.exp2(old - best))
                    if slot < 2:
                        top[m, h, here, :] = best
                    packed.append(jnp.concatenate(
                        [jnp.exp2(p - best).astype(jnp.bfloat16) for p in parts], axis=1))
                blended = dot(jnp.concatenate(packed, axis=0), v_s[h])
                if slot > 0:
                    fade = jnp.concatenate(fades, axis=0)
                    blended = blended + acc[m, h] * jnp.concatenate([fade, fade], axis=1)
                if slot < 2:
                    acc[m, h] = blended
                else:
                    att[h, m] = (blended[:, :head] / blended[:, head:]).astype(jnp.bfloat16)
            return carry

        lax.fori_loop(0, HEADS // together, body, 0)

    inner = up.shape[1]
    cut = width

    def expand(m):
        blended = jnp.concatenate([att[h, m] for h in range(HEADS)], axis=1)
        middle = (xs[0, m].astype(jnp.float32) + dot(blended, wo[...])).astype(jnp.bfloat16)
        mid[m] = middle
        normed = norm_rows(middle, gain2[...].reshape(1, width))
        for c in range(inner // cut):
            hid[m, :, c * cut:(c + 1) * cut] = gelu(
                dot(normed, up[:, c * cut:(c + 1) * cut])).astype(jnp.bfloat16)

    def finish(m):
        out_ref[m] = (mid[m].astype(jnp.float32) + dot(hid[m], down[...])).astype(jnp.bfloat16)

    count = len(pieces)
    late = count // 2
    def far_here(m):
        for t in range(tiles):
            to_onward[m * tiles + t].wait_recv()

    pass_near(0)
    pass_pieces(0, 1)

    have_weight(0)
    x_local.wait()
    project(0, 0)
    pass_pieces(1, 2)
    attend(0, 0)
    pass_near(1)
    project(0, 1)
    pass_pieces(2, late - 1)
    attend(0, 1)
    pass_pieces(late - 1, late)
    project(1, 0)
    attend(1, 0)
    pass_pieces(late, late + 1)
    far_here(0)
    project(2, 0)
    pass_pieces(late + 1, late + 2)
    pass_near(2)
    attend(2, 0)
    pass_pieces(late + 2, late + 3)
    have_weight(1)
    have_weight(2)
    expand(0)
    pass_pieces(late + 3, count)
    project(1, 1)
    attend(1, 1)
    far_here(1)
    project(2, 1)
    attend(2, 1)
    pass_near(3)
    expand(1)
    have_weight(3)
    stores = []
    for m in range(members):
        finish(m)
    for copy in stores:
        copy.wait()
    for copy in to_partner + to_onward + to_twin:
        copy.wait_send()
    for w in range(4):
        for copy in to_across[w] + to_side[w] + near_pass[w] + far_pass[w]:
            copy.wait_send()


def solution(mesh):
    ring, party = mesh.shape["mesh"], mesh.shape["member"]

    def on_device(node_states, projection, output_weight, up_weight, down_weight,
                  attention_gain, feedforward_gain, tile_lists, tile_counts):
        members, rows, width = node_states.shape
        tiles = tile_lists.shape[0]
        head = width // HEADS
        inner = up_weight.shape[1]
        hbm = pl.BlockSpec(memory_space=pltpu.HBM)
        bf16, f32 = jnp.bfloat16, jnp.float32
        copies = members * tiles
        lanes = 1 + 4 * (party // 2 - 1)
        return pl.pallas_call(
            functools.partial(kernel, ring, party, tiles),
            out_shape=pltpu.VMEM(node_states.shape, bf16),
            in_specs=[hbm] * 9,
            out_specs=pl.BlockSpec(memory_space=pltpu.VMEM),
            scratch_shapes=[
                pltpu.VMEM((3, members, rows, width), bf16),
                pltpu.VMEM((width, 3 * width), bf16),
                pltpu.VMEM((width, width), bf16),
                pltpu.VMEM((width, inner), bf16),
                pltpu.VMEM((inner, width), bf16),
                pltpu.VMEM((members, HEADS, rows, head), bf16),
                pltpu.VMEM((HEADS, rows, head), bf16),
                pltpu.VMEM((HEADS, rows, 2 * head), bf16),
                pltpu.VMEM((members, HEADS, rows, 2 * head), f32),
                pltpu.VMEM((members, HEADS, rows, head), f32),
                pltpu.VMEM((HEADS, members, rows, head), bf16),
                pltpu.VMEM((members, rows, inner), bf16),
                pltpu.VMEM((members, rows, width), bf16),
                pltpu.SMEM((tiles, 3 * tiles), f32),
                pltpu.VMEM((width,), f32),
                pltpu.VMEM((width,), f32),
                pltpu.SMEM(tile_lists.shape, jnp.int32),
                pltpu.SMEM(tile_counts.shape, jnp.int32),
                pltpu.SemaphoreType.DMA((9 + members,)),
                pltpu.SemaphoreType.DMA((copies,)),
                pltpu.SemaphoreType.DMA((copies,)),
                pltpu.SemaphoreType.DMA((copies,)),
                pltpu.SemaphoreType.DMA((copies,)),
                pltpu.SemaphoreType.DMA((4 * lanes,)),
                pltpu.SemaphoreType.DMA((4 * lanes,)),
            ],
            compiler_params=pltpu.CompilerParams(
                collective_id=0, has_side_effects=True, vmem_limit_bytes=60000000
            ),
        )(node_states, projection, output_weight, up_weight, down_weight,
          attention_gain, feedforward_gain, tile_lists, tile_counts)

    in_specs = (
        P("member", "mesh", None), P("member", None), P("member", None),
        P("member", None), P("member", None), P(), P(), P("mesh", None), P("mesh"),
    )
    return jax.shard_map(
        on_device, mesh=mesh, in_specs=in_specs,
        out_specs=P("member", "mesh", None), check_vma=False)
```

```python
import functools
import math

import jax
import jax.numpy as jnp
from jax import lax
from jax.experimental import pallas as pl
from jax.experimental.pallas import tpu as pltpu
from jax.sharding import PartitionSpec as P

HEADS = 4
RIM_T = 4
MESH = pl.DeviceIdType.MESH
MASKED = -1e30
EPS = 1e-05
SLOTS = 42
PROJ_VIA = (None, None, None, None)
UP_CUTS = 2
DOWN_SHARED = 12
DOWN_CUTS = 3
PIECES = 2
CUT = 256
ORDER = [[(0, 0), (0, 1), (0, 2), (0, 3), (1, 0), (1, 1), (1, 2), (1, 3), (2, 0), (2, 1), (2, 2), (2, 3)], [(0, 0), (0, 1), (0, 2), (0, 3), (1, 0), (1, 1), (1, 2), (2, 0), (2, 1), (1, 3), (2, 2), (2, 3)]]


def norm_rows(rows, gain):
    values = rows.astype(jnp.float32)
    center = values - jnp.mean(values, axis=-1, keepdims=True)
    spread = jnp.mean(center * center, axis=-1, keepdims=True)
    return (center * lax.rsqrt(spread + EPS) * gain).astype(jnp.bfloat16)


def gelu(value):
    inner = math.sqrt(2.0 / math.pi) * (value + 0.044715 * value * value * value)
    return 0.5 * value * (1.0 + jnp.tanh(inner))


def dot(a, b):
    return jnp.dot(a, b, preferred_element_type=jnp.float32)


def kernel(
    ring, party, tiles,
    x_hbm, proj_hbm, wo_hbm, up_hbm, down_hbm, gain1_hbm, gain2_hbm, lists_hbm, counts_hbm,
    out_ref,
    xs, xn, wproj, wo, up, down, q_s, k_s, v_s, acc, top, att, hid, mid, nrm, bias,
    gain1, gain2, lists, counts,
    local_sem, xp_send, xp_recv, xf_send, xf_recv, w_send, w_recv,
):
    members, rows, width = x_hbm.shape
    tile = rows // tiles
    head = width // HEADS
    groups = party // 2
    inner = up.shape[1]
    me = lax.axis_index("mesh")
    mine = lax.axis_index("member")
    parity = lax.rem(me, 2)
    side = 1 - 2 * parity
    partner = me + side
    onward = lax.rem(me + 2 * side + ring, ring)
    behind = lax.rem(me - 2 * side + ring, ring)
    core = lax.rem(mine, 2)
    twin = mine + 1 - 2 * core
    across = [lax.rem(mine + 2 * d, party) for d in range(1, groups)]

    w_local = []

    def part(ref, who, depth, start, size):
        return ref.at[pl.ds(pl.multiple_of(who * depth + start, 16), size)]

    small = [pltpu.make_async_copy(src, dst, local_sem.at[i]) for i, (src, dst) in enumerate(
        ((lists_hbm, lists), (counts_hbm, counts), (gain1_hbm, gain1), (gain2_hbm, gain2)))]
    for copy in small:
        copy.start()
    x_local = pltpu.make_async_copy(x_hbm, xs.at[0], local_sem.at[4])
    x_local.start()

    barrier = pltpu.get_barrier_semaphore()
    for peer in (partner, onward, behind):
        pl.semaphore_signal(barrier, inc=1, device_id={"mesh": peer}, device_id_type=MESH)
    for peer in [twin] + across:
        pl.semaphore_signal(barrier, inc=1, device_id={"member": peer}, device_id_type=MESH)

    local_count = [5]

    def local(src, dst):
        copy = pltpu.make_async_copy(src, dst, local_sem.at[local_count[0]])
        local_count[0] += 1
        copy.start()
        return copy

    def head_blocks(h, who, start, size):
        depth = proj_hbm.shape[0]
        return [(proj_hbm.at[pl.ds(start, size), pl.ds(j * width + h * head, head)],
                 wproj.at[h, pl.ds(pl.multiple_of(who * depth + start, 16), size),
                          pl.ds(j * head, head)]) for j in range(3)]

    def row_blocks(shard, whole, who, start, size):
        return [(shard.at[pl.ds(start, size)], part(whole, who, shard.shape[0], start, size))]

    def blocks_of(unit, who, start, size):
        kind, h = unit
        if kind == "proj":
            return head_blocks(h, who, start, size)
        shard, whole = {"wo": (wo_hbm, wo), "up": (up_hbm, up), "down": (down_hbm, down)}[kind]
        return row_blocks(shard, whole, who, start, size)

    proj_local = []
    for h in range(HEADS):
        for s, d in head_blocks(h, mine, 0, proj_hbm.shape[0]):
            pltpu.make_async_copy(s, d, local_sem.at[8 + h]).start()
        whole = wproj.at[h, pl.ds(0, proj_hbm.shape[0])]
        proj_local.append([pltpu.make_async_copy(whole, whole, local_sem.at[8 + h])])
    rest_local = {name: local(shard, part(whole, mine, shard.shape[0], 0, shard.shape[0]))
                  for name, shard, whole in
                  (("wo", wo_hbm, wo), ("up", up_hbm, up), ("down", down_hbm, down))}

    used = [0]
    moved = [0] * 5

    odd = lax.rem(me // 2, 2)
    beside = me + 2 - 4 * odd

    class Stream:
        def __init__(self, way, pairs, target):
            self.pairs, self.way = pairs, way
            self.index = used[0]
            used[0] += 1
            self.size = sum(math.prod(s.shape) for s, _ in pairs) // width
            moved[way] += self.size
            self.target = target

        def copy(self, src, dst):
            return pltpu.make_async_remote_copy(
                src_ref=src, dst_ref=dst, send_sem=w_send.at[self.way],
                recv_sem=w_recv.at[self.index], device_id=self.target, device_id_type=MESH)

        def start(self):
            for s, d in self.pairs:
                self.copy(s, d).start()

        def wait_recv(self):
            whole = down.at[pl.ds(0, self.size)]
            self.copy(whole, whole).wait_recv()

    class Unit:
        def __init__(self, name, start, size, via=None):
            over_pairs, near_pairs, mate_pairs, far_pairs = [], [], [], []
            self.twin = [Stream(0, blocks_of(name, mine, start, size), {"member": twin})]
            self.over, self.near, self.mate, self.far = [], [], [], []
            for d in range(1, groups):
                giver = lax.rem(mine + party - 2 * d, party)
                if via is None:
                    got, part_size = start, size
                else:
                    pick, mate = (odd, beside) if via == "z" else (parity, partner)
                    part_size = size // 2
                    got = pl.multiple_of(start + pick * part_size, 16)
                    other = pl.multiple_of(start + (1 - pick) * part_size, 16)
                self.over.append(Stream(1, blocks_of(name, mine, got, part_size),
                                        {"member": across[d - 1]}))
                here = [(t, t) for _, t in blocks_of(name, giver, got, part_size)]
                self.near.append(Stream(2, here, {"member": twin}))
                if via is not None:
                    self.mate.append(Stream(3, here, {"mesh": mate}))
                    self.far.append(Stream(
                        4, [(t, t) for _, t in blocks_of(name, giver, other, part_size)],
                        {"member": twin}))

        def send_twin(self):
            for stream in self.twin:
                stream.start()

        def send_over(self):
            for stream in self.over:
                stream.start()

        def pass_near(self):
            for stream in self.over:
                stream.wait_recv()
            for stream in self.mate + self.near:
                stream.start()

        def pass_far(self):
            for stream in self.mate:
                stream.wait_recv()
            for stream in self.far:
                stream.start()

        def have(self):
            for stream in self.twin + self.near + self.far:
                stream.wait_recv()

    deep = proj_hbm.shape[0]
    proj_units = [Unit(("proj", h), 0, deep, PROJ_VIA[h]) for h in range(HEADS)]
    wo_units = [Unit(("wo", 0), 0, wo_hbm.shape[0])]
    up_depth = up_hbm.shape[0]
    up_units = [Unit(("up", 0), i * up_depth // UP_CUTS, up_depth // UP_CUTS)
                for i in range(UP_CUTS)]
    down_depth = down_hbm.shape[0]
    shared = down_depth * DOWN_SHARED // 16
    down_shared = [Unit(("down", 0), i * shared // DOWN_CUTS, shared // DOWN_CUTS, "y")
                   for i in range(DOWN_CUTS)] if shared else []
    down_direct = [Unit(("down", 0), shared + i * (down_depth - shared) // 2,
                        (down_depth - shared) // 2) for i in range(2)]
    down_units = down_shared + down_direct
    all_units = proj_units + wo_units + up_units + down_units

    piece = tile // PIECES
    steps = [(m, i * piece) for m in range(members) for i in range(rows // piece)]
    to_partner, to_onward = [], []
    for i, (m, start) in enumerate(steps):
        to_partner.append(pltpu.make_async_remote_copy(
            src_ref=x_hbm.at[m, pl.ds(start, piece)], dst_ref=xs.at[1, m, pl.ds(start, piece)],
            send_sem=xp_send, recv_sem=xp_recv.at[i],
            device_id={"mesh": partner}, device_id_type=MESH))
        to_onward.append(pltpu.make_async_remote_copy(
            src_ref=xs.at[1, m, pl.ds(start, piece)], dst_ref=xs.at[2, m, pl.ds(start, piece)],
            send_sem=xf_send, recv_sem=xf_recv.at[i],
            device_id={"mesh": onward}, device_id_type=MESH))

    pl.semaphore_wait(barrier, 4 + len(across))

    proj_units[0].send_over()
    to_partner[0].start()
    proj_units[0].send_twin()
    for copy in to_partner[1:]:
        copy.start()
    for unit in proj_units[1:]:
        unit.send_over()
        unit.send_twin()
    for unit in wo_units + up_units + down_units:
        unit.send_over()
    for unit in wo_units + up_units + down_units:
        unit.send_twin()

    for m in range(members):
        v_s[m, :, :, head:] = jnp.ones(v_s.shape[1:3] + (head,), jnp.bfloat16)

    for copy in small:
        copy.wait()

    every = tiles * ring
    first_tile = me * tiles

    def fill_bias(t, carry):
        count = counts[t]
        places = []
        for j in range(lists.shape[1]):
            place = lists[t, j] - first_tile + RIM_T
            place = jnp.where(place < 0, place + every, place)
            place = jnp.where(place >= every, place - every, place)
            places.append(jnp.where(j < count, place, -1))
        for c in range(3 * tiles):
            if c < tiles:
                want = RIM_T + c
            elif c < 2 * tiles:
                want = jnp.where(parity == 0, RIM_T + tiles + c - tiles, RIM_T - tiles + c - tiles)
            else:
                want = jnp.where(parity == 0, RIM_T - tiles + c - 2 * tiles, RIM_T + tiles + c - 2 * tiles)
            hit = places[0] == want
            for place in places[1:]:
                hit = jnp.logical_or(hit, place == want)
            bias[t, c] = jnp.where(hit, 0.0, MASKED)
        return carry

    lax.fori_loop(0, tiles, fill_bias, 0)

    query_scale = math.log2(math.e) / math.sqrt(head)
    x_local.wait()

    def norm_own(m):
        xn[m] = norm_rows(xs[0, m], gain1[...].reshape(1, width))

    def project_own(h):
        both = xn[...].reshape(members * rows, width)
        made = dot(both, wproj[h])
        for m in range(members):
            here = slice(m * rows, (m + 1) * rows)
            q_s[m, h] = (made[here, :head] * query_scale).astype(jnp.bfloat16)
            k_s[m, h, :rows] = made[here, head:2 * head].astype(jnp.bfloat16)
            v_s[m, h, :rows, :head] = made[here, 2 * head:].astype(jnp.bfloat16)

    def project_rim(m, lo, hi):
        while lo < hi:
            slot, at = ORDER[m][lo]
            end = lo + 1
            while end < hi and ORDER[m][end] == (slot, at + end - lo):
                end += 1
            place = slice(lo * tile, end * tile)
            normed = norm_rows(xs[slot, m, at * tile:(at + end - lo) * tile],
                               gain1[...].reshape(1, width))
            for h in range(HEADS):
                made = dot(normed, wproj[h, :, head:]).astype(jnp.bfloat16)
                k_s[m, h, place] = made[:, :head]
                v_s[m, h, place, :head] = made[:, head:]
            lo = end

    def score(m, h, lo, hi):
        return lax.dot_general(
            q_s[m, h], k_s[m, h, lo * tile:hi * tile], (((1,), (1,)), ((), ())),
            preferred_element_type=jnp.float32)

    def weigh(m, h, lo, hi, last, scores):
        marks = [[bias[t, ORDER[m][c][0] * tiles + ORDER[m][c][1]] for c in range(lo, hi)]
                 for t in range(tiles)]
        packed, fades = [], []
        for t in range(tiles):
            here = slice(t * tile, (t + 1) * tile)
            parts = [scores[here, c * tile:(c + 1) * tile] + marks[t][c] for c in range(hi - lo)]
            best = parts[0]
            for p in parts[1:]:
                best = jnp.maximum(best, p)
            best = jnp.broadcast_to(jnp.max(best, axis=-1, keepdims=True), (tile, tile))
            if lo > 0:
                old = top[m, h, here, :]
                best = jnp.maximum(best, old)
                fades.append(jnp.exp2(old - best))
            if not last:
                top[m, h, here, :] = best
            packed.append(jnp.concatenate(
                [jnp.exp2(p - best).astype(jnp.bfloat16) for p in parts], axis=1))
        blended = dot(jnp.concatenate(packed, axis=0), v_s[m, h, lo * tile:hi * tile])
        if lo > 0:
            fade = jnp.concatenate(fades, axis=0)
            blended = blended + acc[m, h] * jnp.concatenate([fade, fade], axis=1)
        if last:
            att[m, h] = (blended[:, :head] / blended[:, head:]).astype(jnp.bfloat16)
        else:
            acc[m, h] = blended

    def attend(pairs, lo, hi, last=False):
        ahead = score(*pairs[0], lo, hi)
        for i, (m, h) in enumerate(pairs):
            scores = ahead
            if i + 1 < len(pairs):
                ahead = score(*pairs[i + 1], lo, hi)
            weigh(m, h, lo, hi, last, scores)

    def heads_of(m):
        return [(m, h) for h in range(HEADS)]

    def mix(m):
        blended = jnp.concatenate([att[m, h] for h in range(HEADS)], axis=1)
        middle = (xs[0, m].astype(jnp.float32) + dot(blended, wo[...])).astype(jnp.bfloat16)
        mid[m] = middle
        nrm[m] = norm_rows(middle, gain2[...].reshape(1, width))

    def expand(m):
        for c in range(inner // CUT):
            cut = slice(c * CUT, (c + 1) * CUT)
            hid[m, :, cut] = gelu(dot(nrm[m], up[:, cut])).astype(jnp.bfloat16)

    def finish(m):
        out_ref[m] = (mid[m].astype(jnp.float32) + dot(hid[m], down[...])).astype(jnp.bfloat16)

    def relay(first, last):
        for i in range(first, last):
            to_partner[i].wait_recv()
            to_onward[i].start()

    def far(first, last):
        for i in range(first, last):
            to_onward[i].wait_recv()

    def have_local(copies):
        for copy in copies:
            copy.wait()

    def near(units):
        for unit in units:
            unit.pass_near()

    def far_weights(units):
        for unit in units:
            unit.pass_far()

    def have(units):
        for unit in units:
            unit.have()


    norm_own(0)
    norm_own(1)
    relay(0, 1)
    near(proj_units[0:1])
    have_local(proj_local[0])
    relay(1, 2)
    have(proj_units[0:1])
    for h in range(HEADS):
        project_own(h)
        relay(h + 2, h + 3)
        if h + 1 < HEADS:
            near(proj_units[h + 1:h + 2])
        attend([(m, h) for m in range(members)], 0, tiles)
        if h + 1 < HEADS:
            have_local(proj_local[h + 1])
            far_weights(proj_units[h + 1:h + 2])
            have(proj_units[h + 1:h + 2])
    relay(6, 8)
    near(wo_units)
    far(0, 4)
    project_rim(0, tiles, tiles + 6)
    relay(8, 9)
    attend(heads_of(0), tiles, tiles + 6)
    relay(9, 11)
    far(4, 8)
    project_rim(0, tiles + 6, 3 * tiles)
    relay(11, 12)
    attend(heads_of(0), tiles + 6, 3 * tiles, True)
    near(up_units[:UP_CUTS // 2])
    have_local([rest_local["wo"]])
    have(wo_units)
    relay(12, 13)
    mix(0)
    relay(13, 14)
    project_rim(1, tiles, tiles + 3)
    attend(heads_of(1), tiles, tiles + 3)
    relay(14, 16)
    far(8, 12)
    project_rim(1, tiles + 3, tiles + 6)
    attend(heads_of(1), tiles + 3, tiles + 6)
    near(up_units[UP_CUTS // 2:])
    near(down_shared)
    have_local([rest_local["up"]])
    have(up_units)
    expand(0)
    far(12, 16)
    project_rim(1, tiles + 6, 3 * tiles)
    attend(heads_of(1), tiles + 6, 3 * tiles, True)
    mix(1)
    far_weights(down_shared)
    near(down_direct)
    expand(1)
    have_local([rest_local["down"]])
    have(down_units)
    for m in range(members):
        finish(m)

    for sem in (xp_send, xf_send):
        pltpu.make_async_remote_copy(
            src_ref=xs.at[1], dst_ref=xs.at[2], send_sem=sem, recv_sem=w_recv.at[0],
            device_id={"mesh": partner}, device_id_type=MESH).wait_send()
    for way, size in enumerate(moved):
        if size:
            whole = down.at[pl.ds(0, size)]
            pltpu.make_async_remote_copy(
                src_ref=whole, dst_ref=whole, send_sem=w_send.at[way], recv_sem=w_recv.at[0],
                device_id={"member": twin}, device_id_type=MESH).wait_send()


def solution(mesh):
    ring, party = mesh.shape["mesh"], mesh.shape["member"]

    def on_device(node_states, projection, output_weight, up_weight, down_weight,
                  attention_gain, feedforward_gain, tile_lists, tile_counts):
        members, rows, width = node_states.shape
        tiles = tile_lists.shape[0]
        head = width // HEADS
        inner = up_weight.shape[1]
        hbm = pl.BlockSpec(memory_space=pltpu.HBM)
        bf16, f32 = jnp.bfloat16, jnp.float32
        copies = members * tiles * PIECES
        keys = 3 * rows
        return pl.pallas_call(
            functools.partial(kernel, ring, party, tiles),
            out_shape=pltpu.VMEM(node_states.shape, bf16),
            in_specs=[hbm] * 9,
            out_specs=pl.BlockSpec(memory_space=pltpu.VMEM),
            scratch_shapes=[
                pltpu.VMEM((3, members, rows, width), bf16),
                pltpu.VMEM((members, rows, width), bf16),
                pltpu.VMEM((HEADS, width, 3 * head), bf16),
                pltpu.VMEM((width, width), bf16),
                pltpu.VMEM((width, inner), bf16),
                pltpu.VMEM((inner, width), bf16),
                pltpu.VMEM((members, HEADS, rows, head), bf16),
                pltpu.VMEM((members, HEADS, keys, head), bf16),
                pltpu.VMEM((members, HEADS, keys, 2 * head), bf16),
                pltpu.VMEM((members, HEADS, rows, 2 * head), f32),
                pltpu.VMEM((members, HEADS, rows, head), f32),
                pltpu.VMEM((members, HEADS, rows, head), bf16),
                pltpu.VMEM((members, rows, inner), bf16),
                pltpu.VMEM((members, rows, width), bf16),
                pltpu.VMEM((members, rows, width), bf16),
                pltpu.SMEM((tiles, 3 * tiles), f32),
                pltpu.VMEM((width,), f32),
                pltpu.VMEM((width,), f32),
                pltpu.SMEM(tile_lists.shape, jnp.int32),
                pltpu.SMEM(tile_counts.shape, jnp.int32),
                pltpu.SemaphoreType.DMA((8 + HEADS,)),
                pltpu.SemaphoreType.DMA,
                pltpu.SemaphoreType.DMA((copies,)),
                pltpu.SemaphoreType.DMA,
                pltpu.SemaphoreType.DMA((copies,)),
                pltpu.SemaphoreType.DMA((5,)),
                pltpu.SemaphoreType.DMA((SLOTS,)),
            ],
            compiler_params=pltpu.CompilerParams(
                collective_id=0, has_side_effects=True, vmem_limit_bytes=60000000
            ),
        )(node_states, projection, output_weight, up_weight, down_weight,
          attention_gain, feedforward_gain, tile_lists, tile_counts)

    in_specs = (
        P("member", "mesh", None), P("member", None), P("member", None),
        P("member", None), P("member", None), P(), P(), P("mesh", None), P("mesh"),
    )
    return jax.shard_map(
        on_device, mesh=mesh, in_specs=in_specs,
        out_specs=P("member", "mesh", None), check_vma=False)
```

```python
import functools
import math

import jax
import jax.numpy as jnp
from jax import lax
from jax.experimental import pallas as pl
from jax.experimental.pallas import tpu as pltpu
from jax.sharding import PartitionSpec as P

HEADS = 4
RIM_T = 4
MESH = pl.DeviceIdType.MESH
MASKED = -1e30
EPS = 1e-05
SLOTS = 24
PROJ_VIA = (None, None, None, None)
UP_CUTS = 4
DOWN_SHARED = 10
DOWN_CUTS = 2
PIECES = 2
CUT = 256
MIX_CUTS = 1
LAST = 2
FAR = [4, 8, 10, 12, 14, 17]
ORDER = [[(0, 0), (0, 1), (0, 2), (0, 3), (1, 0), (1, 1), (1, 2), (1, 3), (2, 0), (2, 1), (2, 2), (2, 3)], [(0, 0), (0, 1), (0, 2), (0, 3), (1, 0), (1, 1), (1, 2), (2, 0), (2, 1), (1, 3), (2, 2), (2, 3)]]


def norm_rows(rows, gain):
    values = rows.astype(jnp.float32)
    center = values - jnp.mean(values, axis=-1, keepdims=True)
    spread = jnp.mean(center * center, axis=-1, keepdims=True)
    return (center * lax.rsqrt(spread + EPS) * gain).astype(jnp.bfloat16)


def twice_gelu(value):
    scale = math.sqrt(2.0 / math.pi)
    inner = value * (value * value * (0.044715 * scale) + scale)
    return (value * jnp.tanh(inner) + value).astype(jnp.bfloat16)


def dot(a, b):
    return jnp.dot(a, b, preferred_element_type=jnp.float32)


def kernel(
    ring, party, tiles,
    x_hbm, proj_hbm, wo_hbm, up_hbm, down_hbm, gain1_hbm, gain2_hbm, lists_hbm, counts_hbm,
    out_ref,
    xs, xn, wproj, wo, up, down, q_s, k_s, v_s, acc, top, att, hid, mid, nrm, part_s, bias,
    gain1, gain2, lists, counts,
    local_sem, xp_send, xp_recv, xf_send, xf_recv, w_send, w_recv,
):
    members, rows, width = x_hbm.shape
    tile = rows // tiles
    head = width // HEADS
    groups = party // 2
    inner = up.shape[1]
    me = lax.axis_index("mesh")
    mine = lax.axis_index("member")
    parity = lax.rem(me, 2)
    side = 1 - 2 * parity
    partner = me + side
    onward = lax.rem(me + 2 * side + ring, ring)
    behind = lax.rem(me - 2 * side + ring, ring)
    core = lax.rem(mine, 2)
    twin = mine + 1 - 2 * core
    across = [lax.rem(mine + 2 * d, party) for d in range(1, groups)]

    def part(ref, who, depth, start, size):
        return ref.at[pl.ds(pl.multiple_of(who * depth + start, 16), size)]

    small = [pltpu.make_async_copy(src, dst, local_sem.at[i]) for i, (src, dst) in enumerate(
        ((lists_hbm, lists), (counts_hbm, counts), (gain1_hbm, gain1), (gain2_hbm, gain2)))]
    for copy in small:
        copy.start()
    x_local = pltpu.make_async_copy(x_hbm, xs.at[0], local_sem.at[4])
    x_local.start()

    barrier = pltpu.get_barrier_semaphore()
    for peer in (partner, onward, behind):
        pl.semaphore_signal(barrier, inc=1, device_id={"mesh": peer}, device_id_type=MESH)
    for peer in [twin] + across:
        pl.semaphore_signal(barrier, inc=1, device_id={"member": peer}, device_id_type=MESH)

    def head_blocks(h, who, start, size):
        depth = proj_hbm.shape[0]
        return [(proj_hbm.at[pl.ds(start, size), pl.ds(j * width + h * head, head)],
                 wproj.at[h, pl.ds(pl.multiple_of(who * depth + start, 16), size),
                          pl.ds(j * head, head)]) for j in range(3)]

    def row_blocks(shard, whole, who, start, size):
        return [(shard.at[pl.ds(start, size)], part(whole, who, shard.shape[0], start, size))]

    def blocks_of(unit, who, start, size):
        kind, h = unit
        if kind == "proj":
            return head_blocks(h, who, start, size)
        shard, whole = {"wo": (wo_hbm, wo), "up": (up_hbm, up), "down": (down_hbm, down)}[kind]
        return row_blocks(shard, whole, who, start, size)

    proj_local = []
    for h in range(HEADS):
        for s, d in head_blocks(h, mine, 0, proj_hbm.shape[0]):
            pltpu.make_async_copy(s, d, local_sem.at[6]).start()
    whole = down.at[pl.ds(0, 3 * proj_hbm.shape[0])]
    proj_local.append([pltpu.make_async_copy(whole, whole, local_sem.at[6])])
    rest_rows = 0
    for shard, whole in ((wo_hbm, wo), (up_hbm, up), (down_hbm, down)):
        pltpu.make_async_copy(
            shard, part(whole, mine, shard.shape[0], 0, shard.shape[0]), local_sem.at[5]).start()
        rest_rows += math.prod(shard.shape) // width
    whole = down.at[pl.ds(0, rest_rows)]
    rest_local = pltpu.make_async_copy(whole, whole, local_sem.at[5])

    groups_of = {}
    moved = [0] * 5

    odd = lax.rem(me // 2, 2)
    beside = me + 2 - 4 * odd

    class Stream:
        def __init__(self, way, pairs, target, group=None):
            self.pairs, self.way = pairs, way
            self.group = groups_of.setdefault(group or len(groups_of), [len(groups_of), 0, False])
            self.index = self.group[0]
            size = sum(math.prod(s.shape) for s, _ in pairs) // width
            self.group[1] += size
            moved[way] += size
            self.target = target

        def copy(self, src, dst):
            return pltpu.make_async_remote_copy(
                src_ref=src, dst_ref=dst, send_sem=w_send.at[self.way],
                recv_sem=w_recv.at[self.index], device_id=self.target, device_id_type=MESH)

        def start(self):
            for s, d in self.pairs:
                self.copy(s, d).start()

        def wait_recv(self):
            if not self.group[2]:
                self.group[2] = True
                whole = down.at[pl.ds(0, self.group[1])]
                self.copy(whole, whole).wait_recv()

    class Unit:
        def __init__(self, name, start, size, via=None):
            over_pairs, near_pairs, mate_pairs, far_pairs = [], [], [], []
            kind = name[0]
            self.twin = [Stream(0, blocks_of(name, mine, start, size), {"member": twin},
                                "own" if kind == "proj" else "own rest")]
            passed = None if kind == "proj" else "passed " + kind
            self.over, self.near, self.mate, self.far = [], [], [], []
            for d in range(1, groups):
                giver = lax.rem(mine + party - 2 * d, party)
                if via is None:
                    got, part_size = start, size
                else:
                    pick, mate = (odd, beside) if via == "z" else (parity, partner)
                    part_size = size // 2
                    got = pl.multiple_of(start + pick * part_size, 16)
                    other = pl.multiple_of(start + (1 - pick) * part_size, 16)
                self.over.append(Stream(1, blocks_of(name, mine, got, part_size),
                                        {"member": across[d - 1]}))
                here = [(t, t) for _, t in blocks_of(name, giver, got, part_size)]
                self.near.append(Stream(2, here, {"member": twin}, passed))
                if via is not None:
                    self.mate.append(Stream(3, here, {"mesh": mate}))
                    self.far.append(Stream(
                        4, [(t, t) for _, t in blocks_of(name, giver, other, part_size)],
                        {"member": twin}, passed))

        def send_twin(self):
            for stream in self.twin:
                stream.start()

        def send_over(self):
            for stream in self.over:
                stream.start()

        def pass_near(self):
            for stream in self.over:
                stream.wait_recv()
            for stream in self.mate + self.near:
                stream.start()

        def pass_far(self):
            for stream in self.mate:
                stream.wait_recv()
            for stream in self.far:
                stream.start()

        def have(self):
            for stream in self.twin + self.near + self.far:
                stream.wait_recv()

    deep = proj_hbm.shape[0]
    proj_units = [Unit(("proj", h), 0, deep, PROJ_VIA[h]) for h in range(HEADS)]
    wo_units = [Unit(("wo", 0), 0, wo_hbm.shape[0])]
    up_depth = up_hbm.shape[0]
    up_units = [Unit(("up", 0), i * up_depth // UP_CUTS, up_depth // UP_CUTS)
                for i in range(UP_CUTS)]
    down_depth = down_hbm.shape[0]
    shared = down_depth * DOWN_SHARED // 16
    down_shared = [Unit(("down", 0), i * shared // DOWN_CUTS, shared // DOWN_CUTS, "y")
                   for i in range(DOWN_CUTS)] if shared else []
    down_direct = [Unit(("down", 0), shared + i * (down_depth - shared) // 2,
                        (down_depth - shared) // 2) for i in range(2)]
    down_units = down_shared + down_direct
    all_units = proj_units + wo_units + up_units + down_units

    piece = tile // PIECES
    steps = [(m, i * piece, piece) for m in range(members) for i in range(rows // piece)]
    m, start, size = steps.pop()
    steps += [(m, start + i * (size // LAST), size // LAST) for i in range(LAST)]
    to_partner, to_onward = [], []
    for i, (m, start, size) in enumerate(steps):
        to_partner.append(pltpu.make_async_remote_copy(
            src_ref=x_hbm.at[m, pl.ds(start, size)], dst_ref=xs.at[1, m, pl.ds(start, size)],
            send_sem=xp_send, recv_sem=xp_recv.at[i],
            device_id={"mesh": partner}, device_id_type=MESH))
        to_onward.append(pltpu.make_async_remote_copy(
            src_ref=xs.at[1, m, pl.ds(start, size)], dst_ref=xs.at[2, m, pl.ds(start, size)],
            send_sem=xf_send, recv_sem=xf_recv.at[FAR.index(next(f for f in FAR if i < f))],
            device_id={"mesh": onward}, device_id_type=MESH))

    pl.semaphore_wait(barrier, 4 + len(across))

    proj_units[0].send_over()
    to_partner[0].start()
    proj_units[0].send_twin()
    for copy in to_partner[1:]:
        copy.start()
    for unit in proj_units[1:]:
        unit.send_over()
        unit.send_twin()
    for unit in wo_units + up_units + down_units:
        unit.send_over()
    for unit in wo_units + up_units + down_units:
        unit.send_twin()

    for m in range(members):
        v_s[m, :, :, head:] = jnp.ones(v_s.shape[1:3] + (head,), jnp.bfloat16)

    for copy in small:
        copy.wait()

    every = tiles * ring
    first_tile = me * tiles

    def fill_bias(t, carry):
        count = counts[t]
        places = []
        for j in range(lists.shape[1]):
            place = lists[t, j] - first_tile + RIM_T
            place = jnp.where(place < 0, place + every, place)
            place = jnp.where(place >= every, place - every, place)
            places.append(jnp.where(j < count, place, -1))
        for c in range(3 * tiles):
            if c < tiles:
                want = RIM_T + c
            elif c < 2 * tiles:
                want = jnp.where(parity == 0, RIM_T + tiles + c - tiles, RIM_T - tiles + c - tiles)
            else:
                want = jnp.where(parity == 0, RIM_T - tiles + c - 2 * tiles, RIM_T + tiles + c - 2 * tiles)
            hit = places[0] == want
            for place in places[1:]:
                hit = jnp.logical_or(hit, place == want)
            bias[t, c] = jnp.where(hit, 0.0, MASKED)
        return carry

    lax.fori_loop(0, tiles, fill_bias, 0)

    query_scale = math.log2(math.e) / math.sqrt(head)
    x_local.wait()

    def norm_own(m):
        xn[m] = norm_rows(xs[0, m], gain1[...].reshape(1, width))

    def project_own(h):
        both = xn[...].reshape(members * rows, width)
        made = dot(both, wproj[h])
        for m in range(members):
            here = slice(m * rows, (m + 1) * rows)
            q_s[m, h] = (made[here, :head] * query_scale).astype(jnp.bfloat16)
            k_s[m, h, :rows] = made[here, head:2 * head].astype(jnp.bfloat16)
            v_s[m, h, :rows, :head] = made[here, 2 * head:].astype(jnp.bfloat16)

    def project_rim(m, lo, hi):
        while lo < hi:
            slot, at = ORDER[m][lo]
            end = lo + 1
            while end < hi and ORDER[m][end] == (slot, at + end - lo):
                end += 1
            place = slice(lo * tile, end * tile)
            normed = norm_rows(xs[slot, m, at * tile:(at + end - lo) * tile],
                               gain1[...].reshape(1, width))
            for h in range(HEADS):
                made = dot(normed, wproj[h, :, head:]).astype(jnp.bfloat16)
                k_s[m, h, place] = made[:, :head]
                v_s[m, h, place, :head] = made[:, head:]
            lo = end

    everyone = (0, tiles)

    def score(m, h, lo, hi, who):
        return lax.dot_general(
            q_s[m, h, who[0] * tile:who[1] * tile], k_s[m, h, lo * tile:hi * tile],
            (((1,), (1,)), ((), ())), preferred_element_type=jnp.float32)

    def weigh(m, h, lo, hi, last, scores, who):
        packed, fades = [], []
        for t in range(who[0], who[1]):
            here = slice(t * tile, (t + 1) * tile)
            mine_rows = slice((t - who[0]) * tile, (t - who[0] + 1) * tile)
            parts = [scores[mine_rows, (c - lo) * tile:(c - lo + 1) * tile]
                     + bias[t, ORDER[m][c][0] * tiles + ORDER[m][c][1]] for c in range(lo, hi)]
            best = parts[0]
            for p in parts[1:]:
                best = jnp.maximum(best, p)
            best = jnp.broadcast_to(jnp.max(best, axis=-1, keepdims=True), (tile, tile))
            if lo > 0:
                old = top[m, h, here, :]
                best = jnp.maximum(best, old)
                fades.append(jnp.exp2(old - best))
            if not last:
                top[m, h, here, :] = best
            packed.append(jnp.concatenate(
                [jnp.exp2(p - best).astype(jnp.bfloat16) for p in parts], axis=1))
        rows_here = slice(who[0] * tile, who[1] * tile)
        blended = dot(jnp.concatenate(packed, axis=0), v_s[m, h, lo * tile:hi * tile])
        if lo > 0:
            fade = jnp.concatenate(fades, axis=0)
            blended = blended + acc[m, h, rows_here] * jnp.concatenate([fade, fade], axis=1)
        if last:
            att[m, h, rows_here] = (blended[:, :head] / blended[:, head:]).astype(jnp.bfloat16)
        else:
            acc[m, h, rows_here] = blended

    def attend_steps(pairs, lo, hi, last=False, who=everyone):
        ahead = [score(*pairs[0], lo, hi, who)]

        def step(i):
            scores = ahead.pop()
            if i + 1 < len(pairs):
                ahead.append(score(*pairs[i + 1], lo, hi, who))
            weigh(*pairs[i], lo, hi, last, scores, who)

        return [functools.partial(step, i) for i in range(len(pairs))]

    def run(*lists):
        order = sorted(((i + 0.5) / len(steps), n, i)
                       for n, steps in enumerate(lists) for i in range(len(steps)))
        for _, n, i in order:
            lists[n][i]()

    def attend(pairs, lo, hi, last=False, who=everyone):
        run(attend_steps(pairs, lo, hi, last, who))

    def heads_of(m):
        return [(m, h) for h in range(HEADS)]

    def mix(m, who=everyone):
        split = (who[1] - who[0]) * tile // MIX_CUTS
        spans = [slice(who[0] * tile + i * split, who[0] * tile + (i + 1) * split)
                 for i in range(MIX_CUTS)]
        mixed = [dot(jnp.concatenate([att[m, h, span] for h in range(HEADS)], axis=1), wo[...])
                 for span in spans]
        for span, value in zip(spans, mixed):
            middle = (xs[0, m, span].astype(jnp.float32) + value).astype(jnp.bfloat16)
            mid[m, span] = middle
            nrm[m, span] = norm_rows(middle, gain2[...].reshape(1, width))

    def expand_steps(m, who=everyone):
        rows_here = slice(who[0] * tile, who[1] * tile)

        def step(c):
            span = slice(c * CUT, (c + 1) * CUT)
            hid[m, rows_here, span] = twice_gelu(dot(nrm[m, rows_here], up[:, span]))

        return [functools.partial(step, c) for c in range(inner // CUT)]

    def expand(m):
        run(expand_steps(m))

    two = 2 * down_hbm.shape[0]
    chip = mine - core
    own_rows = pl.ds(pl.multiple_of(chip * down_hbm.shape[0], 128), two)
    far_rows = [pl.ds(pl.multiple_of(lax.rem(chip + 2 * d, party) * down_hbm.shape[0], 128), two)
                for d in range(1, groups)]

    def begin_steps(m, who=everyone):
        rows_here = slice(who[0] * tile, who[1] * tile)

        def step(c):
            span = slice(c * 256, (c + 1) * 256)
            part_s[m, rows_here, span] = (2.0 * mid[m, rows_here, span].astype(jnp.float32)
                                          + dot(hid[m, rows_here, own_rows], down[own_rows, span]))

        return [functools.partial(step, c) for c in range(width // 256)]

    def end_steps(m):
        def step(c):
            span = slice(c * 256, (c + 1) * 256)
            total = part_s[m, :, span]
            for there in far_rows:
                total = total + dot(hid[m, :, there], down[there, span])
            out_ref[m, :, span] = (0.5 * total).astype(jnp.bfloat16)

        return [functools.partial(step, c) for c in range(width // 256)]

    def relay(first, last):
        for i in range(first, last):
            to_partner[i].wait_recv()
            to_onward[i].start()

    def far(last):
        n = FAR.index(last)
        rows_in = sum(size for _, _, size in steps[FAR[n - 1] if n else 0:last])
        whole = down.at[pl.ds(0, rows_in)]
        pltpu.make_async_remote_copy(
            src_ref=whole, dst_ref=whole, send_sem=xf_send, recv_sem=xf_recv.at[n],
            device_id={"mesh": onward}, device_id_type=MESH).wait_recv()

    def have_local(copies):
        for copy in copies:
            copy.wait()

    def near(units):
        for unit in units:
            unit.pass_near()

    def far_weights(units):
        for unit in units:
            unit.pass_far()

    def have(units):
        for unit in units:
            unit.have()


    norm_own(0)
    norm_own(1)
    relay(0, 1)
    near(proj_units[0:1])
    have_local(proj_local[0])
    relay(1, 2)
    have(proj_units[0:1])
    for h in range(HEADS):
        project_own(h)
        if h + 1 < HEADS:
            if h == 1:
                relay(3, 4)
            near(proj_units[h + 1:h + 2])
            if h == 0:
                relay(2, 3)
            if h == 2:
                relay(5, 6)
        if h == 3:
            relay(6, 7)
        attend([(m, h) for m in range(members)], 0, tiles)
        if h + 1 < HEADS:
            if h == 1:
                relay(4, 5)
            have(proj_units[h + 1:h + 2])
    relay(7, 8)
    near(wo_units)
    far(4)
    project_rim(0, tiles, tiles + 6)
    relay(8, 9)
    attend(heads_of(0), tiles, tiles + 6)
    relay(9, 10)
    project_rim(1, tiles, tiles + 1)
    have_local([rest_local])
    have(wo_units)
    relay(10, 11)
    far(8)
    project_rim(0, tiles + 6, 3 * tiles)
    relay(11, 12)
    near(up_units[:1])
    attend(heads_of(0), tiles + 6, 3 * tiles, True)
    project_rim(1, tiles + 1, tiles + 2)
    mix(0)
    relay(12, 13)
    near(up_units[1:2])
    attend(heads_of(1), tiles, tiles + 2)
    relay(13, 14)
    far(10)
    project_rim(1, tiles + 2, tiles + 4)
    near(up_units[2:3])
    attend(heads_of(1), tiles + 2, tiles + 4)
    relay(14, 15)
    near(up_units[3:])
    relay(15, 15 + LAST)
    far(12)
    project_rim(1, tiles + 4, tiles + 6)
    attend(heads_of(1), tiles + 4, tiles + 6)
    have(up_units)
    near(down_shared[:1])
    expand(0)
    near(down_shared[1:])
    run(begin_steps(0))
    far(14)
    project_rim(1, tiles + 6, tiles + 7)
    far(15 + LAST)
    project_rim(1, tiles + 7, 3 * tiles)
    half = tiles // 2
    first, second = (0, half), (half, tiles)
    attend(heads_of(1), tiles + 6, 3 * tiles, True, first)
    far_weights(down_shared[:1])
    near(down_direct[:1])
    mix(1, first)
    run(attend_steps(heads_of(1), tiles + 6, 3 * tiles, True, second), expand_steps(1, first)[:4])
    far_weights(down_shared[1:])
    near(down_direct[1:])
    mix(1, second)
    run(expand_steps(1, first)[4:], expand_steps(1, second)[:4])
    run(begin_steps(1, first), expand_steps(1, second)[4:])
    run(begin_steps(1, second))
    have(down_units)
    run(end_steps(0), end_steps(1))

    for sem in (xp_send, xf_send):
        pltpu.make_async_remote_copy(
            src_ref=xs.at[1], dst_ref=xs.at[2], send_sem=sem, recv_sem=w_recv.at[0],
            device_id={"mesh": partner}, device_id_type=MESH).wait_send()
    for way, size in enumerate(moved):
        if size:
            whole = down.at[pl.ds(0, size)]
            pltpu.make_async_remote_copy(
                src_ref=whole, dst_ref=whole, send_sem=w_send.at[way], recv_sem=w_recv.at[0],
                device_id={"member": twin}, device_id_type=MESH).wait_send()


def solution(mesh):
    ring, party = mesh.shape["mesh"], mesh.shape["member"]

    def on_device(node_states, projection, output_weight, up_weight, down_weight,
                  attention_gain, feedforward_gain, tile_lists, tile_counts):
        members, rows, width = node_states.shape
        tiles = tile_lists.shape[0]
        head = width // HEADS
        inner = up_weight.shape[1]
        hbm = pl.BlockSpec(memory_space=pltpu.HBM)
        bf16, f32 = jnp.bfloat16, jnp.float32
        copies = members * tiles * PIECES + LAST - 1
        keys = 3 * rows
        return pl.pallas_call(
            functools.partial(kernel, ring, party, tiles),
            out_shape=pltpu.VMEM(node_states.shape, bf16),
            in_specs=[hbm] * 9,
            out_specs=pl.BlockSpec(memory_space=pltpu.VMEM),
            scratch_shapes=[
                pltpu.VMEM((3, members, rows, width), bf16),
                pltpu.VMEM((members, rows, width), bf16),
                pltpu.VMEM((HEADS, width, 3 * head), bf16),
                pltpu.VMEM((width, width), bf16),
                pltpu.VMEM((width, inner), bf16),
                pltpu.VMEM((inner, width), bf16),
                pltpu.VMEM((members, HEADS, rows, head), bf16),
                pltpu.VMEM((members, HEADS, keys, head), bf16),
                pltpu.VMEM((members, HEADS, keys, 2 * head), bf16),
                pltpu.VMEM((members, HEADS, rows, 2 * head), f32),
                pltpu.VMEM((members, HEADS, rows, head), f32),
                pltpu.VMEM((members, HEADS, rows, head), bf16),
                pltpu.VMEM((members, rows, inner), bf16),
                pltpu.VMEM((members, rows, width), bf16),
                pltpu.VMEM((members, rows, width), bf16),
                pltpu.VMEM((members, rows, width), f32),
                pltpu.SMEM((tiles, 3 * tiles), f32),
                pltpu.VMEM((width,), f32),
                pltpu.VMEM((width,), f32),
                pltpu.SMEM(tile_lists.shape, jnp.int32),
                pltpu.SMEM(tile_counts.shape, jnp.int32),
                pltpu.SemaphoreType.DMA((7,)),
                pltpu.SemaphoreType.DMA,
                pltpu.SemaphoreType.DMA((copies,)),
                pltpu.SemaphoreType.DMA,
                pltpu.SemaphoreType.DMA((len(FAR),)),
                pltpu.SemaphoreType.DMA((5,)),
                pltpu.SemaphoreType.DMA((SLOTS,)),
            ],
            compiler_params=pltpu.CompilerParams(
                collective_id=0, has_side_effects=True, vmem_limit_bytes=60000000
            ),
        )(node_states, projection, output_weight, up_weight, down_weight,
          attention_gain, feedforward_gain, tile_lists, tile_counts)

    in_specs = (
        P("member", "mesh", None), P("member", None), P("member", None),
        P("member", None), P("member", None), P(), P(), P("mesh", None), P("mesh"),
    )
    return jax.shard_map(
        on_device, mesh=mesh, in_specs=in_specs,
        out_specs=P("member", "mesh", None), check_vma=False)
```

```python
import functools
import math

import jax
import jax.numpy as jnp
from jax import lax
from jax.experimental import pallas as pl
from jax.experimental.pallas import tpu as pltpu
from jax.sharding import PartitionSpec as P

HEADS = 4
RIM_T = 4
MESH = pl.DeviceIdType.MESH
MASKED = -1e30
EPS = 1e-05
SLOTS = 24
PROJ_VIA = (None, None, None, None)
UP_CUTS = 4
DOWN_SHARED = 10
DOWN_CUTS = 2
PIECES = 2
CUT = 256
MIX_CUTS = 1
LAST = 2
FAR = [4, 8, 10, 12, 14, 17]
ORDER = [[(0, 0), (0, 1), (0, 2), (0, 3), (1, 0), (1, 1), (1, 2), (1, 3), (2, 0), (2, 1), (2, 2), (2, 3)], [(0, 0), (0, 1), (0, 2), (0, 3), (1, 0), (1, 1), (1, 2), (2, 0), (2, 1), (1, 3), (2, 2), (2, 3)]]


def norm_rows(rows, gain):
    values = rows.astype(jnp.float32)
    center = values - jnp.mean(values, axis=-1, keepdims=True)
    spread = jnp.mean(center * center, axis=-1, keepdims=True)
    return (center * lax.rsqrt(spread + EPS) * gain).astype(jnp.bfloat16)


def twice_gelu(value):
    scale = math.sqrt(2.0 / math.pi)
    inner = value * (value * value * (0.044715 * scale) + scale)
    return (value * jnp.tanh(inner) + value).astype(jnp.bfloat16)


def dot(a, b):
    return jnp.dot(a, b, preferred_element_type=jnp.float32)


def kernel(
    ring, party, tiles,
    x_hbm, proj_hbm, wo_hbm, up_hbm, down_hbm, gain1_hbm, gain2_hbm, lists_hbm, counts_hbm,
    out_ref,
    xs, xn, wproj, wo, up, down, q_s, k_s, v_s, acc, top, att, hid, mid, nrm, part_s, bias,
    gain1, gain2, lists, counts,
    local_sem, xp_send, xp_recv, xf_send, xf_recv, w_send, w_recv,
):
    members, rows, width = x_hbm.shape
    tile = rows // tiles
    head = width // HEADS
    groups = party // 2
    inner = up.shape[1]
    me = lax.axis_index("mesh")
    mine = lax.axis_index("member")
    parity = lax.rem(me, 2)
    side = 1 - 2 * parity
    partner = me + side
    onward = lax.rem(me + 2 * side + ring, ring)
    behind = lax.rem(me - 2 * side + ring, ring)
    core = lax.rem(mine, 2)
    twin = mine + 1 - 2 * core
    across = [lax.rem(mine + 2 * d, party) for d in range(1, groups)]

    def part(ref, who, depth, start, size):
        return ref.at[pl.ds(pl.multiple_of(who * depth + start, 16), size)]

    small = [pltpu.make_async_copy(src, dst, local_sem.at[i]) for i, (src, dst) in enumerate(
        ((lists_hbm, lists), (counts_hbm, counts), (gain1_hbm, gain1), (gain2_hbm, gain2)))]
    for copy in small:
        copy.start()
    x_local = pltpu.make_async_copy(x_hbm, xs.at[0], local_sem.at[4])
    x_local.start()

    barrier = pltpu.get_barrier_semaphore()
    for peer in (partner, onward, behind):
        pl.semaphore_signal(barrier, inc=1, device_id={"mesh": peer}, device_id_type=MESH)
    for peer in [twin] + across:
        pl.semaphore_signal(barrier, inc=1, device_id={"member": peer}, device_id_type=MESH)

    def head_blocks(h, who, start, size):
        depth = proj_hbm.shape[0]
        return [(proj_hbm.at[pl.ds(start, size), pl.ds(j * width + h * head, head)],
                 wproj.at[h, pl.ds(pl.multiple_of(who * depth + start, 16), size),
                          pl.ds(j * head, head)]) for j in range(3)]

    def row_blocks(shard, whole, who, start, size):
        return [(shard.at[pl.ds(start, size)], part(whole, who, shard.shape[0], start, size))]

    def blocks_of(unit, who, start, size):
        kind, h = unit
        if kind == "proj":
            return head_blocks(h, who, start, size)
        shard, whole = {"wo": (wo_hbm, wo), "up": (up_hbm, up), "down": (down_hbm, down)}[kind]
        return row_blocks(shard, whole, who, start, size)

    proj_local = []
    for h in range(HEADS):
        for s, d in head_blocks(h, mine, 0, proj_hbm.shape[0]):
            pltpu.make_async_copy(s, d, local_sem.at[6]).start()
    whole = down.at[pl.ds(0, 3 * proj_hbm.shape[0])]
    proj_local.append([pltpu.make_async_copy(whole, whole, local_sem.at[6])])
    rest_rows = 0
    for shard, whole in ((wo_hbm, wo), (up_hbm, up), (down_hbm, down)):
        pltpu.make_async_copy(
            shard, part(whole, mine, shard.shape[0], 0, shard.shape[0]), local_sem.at[5]).start()
        rest_rows += math.prod(shard.shape) // width
    whole = down.at[pl.ds(0, rest_rows)]
    rest_local = pltpu.make_async_copy(whole, whole, local_sem.at[5])

    groups_of = {}
    moved = [0] * 5

    odd = lax.rem(me // 2, 2)
    beside = me + 2 - 4 * odd

    class Stream:
        def __init__(self, way, pairs, target, group=None):
            self.pairs, self.way = pairs, way
            self.group = groups_of.setdefault(group or len(groups_of), [len(groups_of), 0, False])
            self.index = self.group[0]
            size = sum(math.prod(s.shape) for s, _ in pairs) // width
            self.group[1] += size
            moved[way] += size
            self.target = target

        def copy(self, src, dst):
            return pltpu.make_async_remote_copy(
                src_ref=src, dst_ref=dst, send_sem=w_send.at[self.way],
                recv_sem=w_recv.at[self.index], device_id=self.target, device_id_type=MESH)

        def start(self):
            for s, d in self.pairs:
                self.copy(s, d).start()

        def wait_recv(self):
            if not self.group[2]:
                self.group[2] = True
                whole = down.at[pl.ds(0, self.group[1])]
                self.copy(whole, whole).wait_recv()

    class Unit:
        def __init__(self, name, start, size, via=None):
            over_pairs, near_pairs, mate_pairs, far_pairs = [], [], [], []
            kind = name[0]
            self.twin = [Stream(0, blocks_of(name, mine, start, size), {"member": twin},
                                "own" if kind == "proj" else "own rest")]
            passed = None if kind == "proj" else "passed " + kind
            self.over, self.near, self.mate, self.far = [], [], [], []
            for d in range(1, groups):
                giver = lax.rem(mine + party - 2 * d, party)
                if via is None:
                    got, part_size = start, size
                else:
                    pick, mate = (odd, beside) if via == "z" else (parity, partner)
                    part_size = size // 2
                    got = pl.multiple_of(start + pick * part_size, 16)
                    other = pl.multiple_of(start + (1 - pick) * part_size, 16)
                self.over.append(Stream(1, blocks_of(name, mine, got, part_size),
                                        {"member": across[d - 1]}))
                here = [(t, t) for _, t in blocks_of(name, giver, got, part_size)]
                self.near.append(Stream(2, here, {"member": twin}, passed))
                if via is not None:
                    self.mate.append(Stream(3, here, {"mesh": mate}))
                    self.far.append(Stream(
                        4, [(t, t) for _, t in blocks_of(name, giver, other, part_size)],
                        {"member": twin}, passed))

        def send_twin(self):
            for stream in self.twin:
                stream.start()

        def send_over(self):
            for stream in self.over:
                stream.start()

        def pass_near(self):
            for stream in self.over:
                stream.wait_recv()
            for stream in self.mate + self.near:
                stream.start()

        def pass_far(self):
            for stream in self.mate:
                stream.wait_recv()
            for stream in self.far:
                stream.start()

        def have(self):
            for stream in self.twin + self.near + self.far:
                stream.wait_recv()

    deep = proj_hbm.shape[0]
    proj_units = [Unit(("proj", h), 0, deep, PROJ_VIA[h]) for h in range(HEADS)]
    wo_units = [Unit(("wo", 0), 0, wo_hbm.shape[0])]
    up_depth = up_hbm.shape[0]
    up_units = [Unit(("up", 0), i * up_depth // UP_CUTS, up_depth // UP_CUTS)
                for i in range(UP_CUTS)]
    down_depth = down_hbm.shape[0]
    shared = down_depth * DOWN_SHARED // 16
    down_shared = [Unit(("down", 0), i * shared // DOWN_CUTS, shared // DOWN_CUTS, "y")
                   for i in range(DOWN_CUTS)] if shared else []
    down_direct = [Unit(("down", 0), shared + i * (down_depth - shared) // 2,
                        (down_depth - shared) // 2) for i in range(2)]
    down_units = down_shared + down_direct
    all_units = proj_units + wo_units + up_units + down_units

    piece = tile // PIECES
    steps = [(m, i * piece, piece) for m in range(members) for i in range(rows // piece)]
    m, start, size = steps.pop()
    steps += [(m, start + i * (size // LAST), size // LAST) for i in range(LAST)]
    to_partner, to_onward = [], []
    for i, (m, start, size) in enumerate(steps):
        to_partner.append(pltpu.make_async_remote_copy(
            src_ref=x_hbm.at[m, pl.ds(start, size)], dst_ref=xs.at[1, m, pl.ds(start, size)],
            send_sem=xp_send, recv_sem=xp_recv.at[i],
            device_id={"mesh": partner}, device_id_type=MESH))
        to_onward.append(pltpu.make_async_remote_copy(
            src_ref=xs.at[1, m, pl.ds(start, size)], dst_ref=xs.at[2, m, pl.ds(start, size)],
            send_sem=xf_send, recv_sem=xf_recv.at[FAR.index(next(f for f in FAR if i < f))],
            device_id={"mesh": onward}, device_id_type=MESH))

    pl.semaphore_wait(barrier, 4 + len(across))

    proj_units[0].send_over()
    to_partner[0].start()
    proj_units[0].send_twin()
    for copy in to_partner[1:]:
        copy.start()
    for unit in proj_units[1:]:
        unit.send_over()
        unit.send_twin()
    for unit in wo_units + up_units + down_units:
        unit.send_over()
    for unit in wo_units + up_units + down_units:
        unit.send_twin()

    for m in range(members):
        v_s[m, :, :, head:] = jnp.ones(v_s.shape[1:3] + (head,), jnp.bfloat16)

    for copy in small:
        copy.wait()

    every = tiles * ring
    first_tile = me * tiles

    def fill_bias(t, carry):
        count = counts[t]
        places = []
        for j in range(lists.shape[1]):
            place = lists[t, j] - first_tile + RIM_T
            place = jnp.where(place < 0, place + every, place)
            place = jnp.where(place >= every, place - every, place)
            places.append(jnp.where(j < count, place, -1))
        for c in range(3 * tiles):
            if c < tiles:
                want = RIM_T + c
            elif c < 2 * tiles:
                want = jnp.where(parity == 0, RIM_T + tiles + c - tiles, RIM_T - tiles + c - tiles)
            else:
                want = jnp.where(parity == 0, RIM_T - tiles + c - 2 * tiles, RIM_T + tiles + c - 2 * tiles)
            hit = places[0] == want
            for place in places[1:]:
                hit = jnp.logical_or(hit, place == want)
            bias[t, c] = jnp.where(hit, 0.0, MASKED)
        return carry

    lax.fori_loop(0, tiles, fill_bias, 0)

    query_scale = math.log2(math.e) / math.sqrt(head)
    x_local.wait()

    def norm_own(m):
        xn[m] = norm_rows(xs[0, m], gain1[...].reshape(1, width))

    def project_own(h):
        both = xn[...].reshape(members * rows, width)
        made = dot(both, wproj[h])
        for m in range(members):
            here = slice(m * rows, (m + 1) * rows)
            q_s[m, h] = (made[here, :head] * query_scale).astype(jnp.bfloat16)
            k_s[m, h, :rows] = made[here, head:2 * head].astype(jnp.bfloat16)
            v_s[m, h, :rows, :head] = made[here, 2 * head:].astype(jnp.bfloat16)

    def project_rim(m, lo, hi):
        while lo < hi:
            slot, at = ORDER[m][lo]
            end = lo + 1
            while end < hi and ORDER[m][end] == (slot, at + end - lo):
                end += 1
            place = slice(lo * tile, end * tile)
            normed = norm_rows(xs[slot, m, at * tile:(at + end - lo) * tile],
                               gain1[...].reshape(1, width))
            for h in range(HEADS):
                made = dot(normed, wproj[h, :, head:]).astype(jnp.bfloat16)
                k_s[m, h, place] = made[:, :head]
                v_s[m, h, place, :head] = made[:, head:]
            lo = end

    everyone = (0, tiles)

    def score(m, h, lo, hi, who):
        return lax.dot_general(
            q_s[m, h, who[0] * tile:who[1] * tile], k_s[m, h, lo * tile:hi * tile],
            (((1,), (1,)), ((), ())), preferred_element_type=jnp.float32)

    def weigh(m, h, lo, hi, last, scores, who):
        packed, fades = [], []
        for t in range(who[0], who[1]):
            here = slice(t * tile, (t + 1) * tile)
            mine_rows = slice((t - who[0]) * tile, (t - who[0] + 1) * tile)
            parts = [scores[mine_rows, (c - lo) * tile:(c - lo + 1) * tile]
                     + bias[t, ORDER[m][c][0] * tiles + ORDER[m][c][1]] for c in range(lo, hi)]
            best = parts[0]
            for p in parts[1:]:
                best = jnp.maximum(best, p)
            best = jnp.broadcast_to(jnp.max(best, axis=-1, keepdims=True), (tile, tile))
            if lo > 0:
                old = top[m, h, here, :]
                best = jnp.maximum(best, old)
                fades.append(jnp.exp2(old - best))
            if not last:
                top[m, h, here, :] = best
            packed.append(jnp.concatenate(
                [jnp.exp2(p - best).astype(jnp.bfloat16) for p in parts], axis=1))
        rows_here = slice(who[0] * tile, who[1] * tile)
        blended = dot(jnp.concatenate(packed, axis=0), v_s[m, h, lo * tile:hi * tile])
        if lo > 0:
            fade = jnp.concatenate(fades, axis=0)
            blended = blended + acc[m, h, rows_here] * jnp.concatenate([fade, fade], axis=1)
        if last:
            att[m, h, rows_here] = (blended[:, :head] / blended[:, head:]).astype(jnp.bfloat16)
        else:
            acc[m, h, rows_here] = blended

    def attend_steps(pairs, lo, hi, last=False, who=everyone):
        ahead = [score(*pairs[0], lo, hi, who)]

        def step(i):
            scores = ahead.pop()
            if i + 1 < len(pairs):
                ahead.append(score(*pairs[i + 1], lo, hi, who))
            weigh(*pairs[i], lo, hi, last, scores, who)

        return [functools.partial(step, i) for i in range(len(pairs))]

    def run(*lists):
        order = sorted(((i + 0.5) / len(steps), n, i)
                       for n, steps in enumerate(lists) for i in range(len(steps)))
        for _, n, i in order:
            lists[n][i]()

    def attend(pairs, lo, hi, last=False, who=everyone):
        run(attend_steps(pairs, lo, hi, last, who))

    def heads_of(m):
        return [(m, h) for h in range(HEADS)]

    def mix(m, who=everyone):
        split = (who[1] - who[0]) * tile // MIX_CUTS
        spans = [slice(who[0] * tile + i * split, who[0] * tile + (i + 1) * split)
                 for i in range(MIX_CUTS)]
        mixed = [dot(jnp.concatenate([att[m, h, span] for h in range(HEADS)], axis=1), wo[...])
                 for span in spans]
        for span, value in zip(spans, mixed):
            middle = (xs[0, m, span].astype(jnp.float32) + value).astype(jnp.bfloat16)
            mid[m, span] = middle
            nrm[m, span] = norm_rows(middle, gain2[...].reshape(1, width))

    def expand_steps(m, who=everyone):
        rows_here = slice(who[0] * tile, who[1] * tile)

        def step(c):
            span = slice(c * CUT, (c + 1) * CUT)
            hid[m, rows_here, span] = twice_gelu(dot(nrm[m, rows_here], up[:, span]))

        return [functools.partial(step, c) for c in range(inner // CUT)]

    def expand(m):
        run(expand_steps(m))

    two = 2 * down_hbm.shape[0]
    chip = mine - core
    own_rows = pl.ds(pl.multiple_of(chip * down_hbm.shape[0], 128), two)
    far_rows = [pl.ds(pl.multiple_of(lax.rem(chip + 2 * d, party) * down_hbm.shape[0], 128), two)
                for d in range(1, groups)]

    def begin_steps(m, who=everyone):
        rows_here = slice(who[0] * tile, who[1] * tile)

        def step(c):
            span = slice(c * 256, (c + 1) * 256)
            part_s[m, rows_here, span] = (2.0 * mid[m, rows_here, span].astype(jnp.float32)
                                          + dot(hid[m, rows_here, own_rows], down[own_rows, span]))

        return [functools.partial(step, c) for c in range(width // 256)]

    def end_steps(m):
        def step(c):
            span = slice(c * 256, (c + 1) * 256)
            total = part_s[m, :, span]
            for there in far_rows:
                total = total + dot(hid[m, :, there], down[there, span])
            out_ref[m, :, span] = (0.5 * total).astype(jnp.bfloat16)

        return [functools.partial(step, c) for c in range(width // 256)]

    def relay(first, last):
        for i in range(first, last):
            to_partner[i].wait_recv()
            to_onward[i].start()

    def far(last):
        n = FAR.index(last)
        rows_in = sum(size for _, _, size in steps[FAR[n - 1] if n else 0:last])
        whole = down.at[pl.ds(0, rows_in)]
        pltpu.make_async_remote_copy(
            src_ref=whole, dst_ref=whole, send_sem=xf_send, recv_sem=xf_recv.at[n],
            device_id={"mesh": onward}, device_id_type=MESH).wait_recv()

    def have_local(copies):
        for copy in copies:
            copy.wait()

    def near(units):
        for unit in units:
            unit.pass_near()

    def far_weights(units):
        for unit in units:
            unit.pass_far()

    def have(units):
        for unit in units:
            unit.have()


    norm_own(0)
    norm_own(1)
    relay(0, 1)
    near(proj_units[0:1])
    have_local(proj_local[0])
    relay(1, 2)
    have(proj_units[0:1])
    for h in range(HEADS):
        project_own(h)
        if h + 1 < HEADS:
            if h == 1:
                relay(3, 4)
            near(proj_units[h + 1:h + 2])
            if h == 0:
                relay(2, 3)
            if h == 2:
                relay(5, 6)
        if h == 3:
            relay(6, 7)
        attend([(m, h) for m in range(members)], 0, tiles)
        if h + 1 < HEADS:
            if h == 1:
                relay(4, 5)
            have(proj_units[h + 1:h + 2])
    relay(7, 8)
    near(wo_units)
    far(4)
    project_rim(0, tiles, tiles + 6)
    relay(8, 9)
    attend(heads_of(0), tiles, tiles + 6)
    relay(9, 10)
    project_rim(1, tiles, tiles + 1)
    have_local([rest_local])
    have(wo_units)
    relay(10, 11)
    far(8)
    project_rim(0, tiles + 6, 3 * tiles)
    relay(11, 12)
    near(up_units[:1])
    attend(heads_of(0), tiles + 6, 3 * tiles, True)
    project_rim(1, tiles + 1, tiles + 2)
    mix(0)
    relay(12, 13)
    near(up_units[1:2])
    attend(heads_of(1), tiles, tiles + 2)
    relay(13, 14)
    far(10)
    project_rim(1, tiles + 2, tiles + 4)
    near(up_units[2:3])
    attend(heads_of(1), tiles + 2, tiles + 4)
    relay(14, 15)
    relay(15, 15 + LAST)
    far(12)
    project_rim(1, tiles + 4, tiles + 6)
    near(up_units[3:])
    attend(heads_of(1), tiles + 4, tiles + 6)
    have(up_units)
    near(down_shared[:1])
    expand(0)
    near(down_shared[1:])
    run(begin_steps(0))
    far(14)
    project_rim(1, tiles + 6, tiles + 7)
    far(15 + LAST)
    project_rim(1, tiles + 7, 3 * tiles)
    half = tiles // 2
    first, second = (0, half), (half, tiles)
    attend(heads_of(1), tiles + 6, 3 * tiles, True, first)
    far_weights(down_shared[:1])
    near(down_direct[:1])
    mix(1, first)
    run(attend_steps(heads_of(1), tiles + 6, 3 * tiles, True, second), expand_steps(1, first)[:4])
    far_weights(down_shared[1:])
    near(down_direct[1:])
    mix(1, second)
    run(expand_steps(1, first)[4:], expand_steps(1, second)[:4])
    run(begin_steps(1, first), expand_steps(1, second)[4:])
    run(begin_steps(1, second))
    have(down_units)
    run(end_steps(0), end_steps(1))

    for sem in (xp_send, xf_send):
        pltpu.make_async_remote_copy(
            src_ref=xs.at[1], dst_ref=xs.at[2], send_sem=sem, recv_sem=w_recv.at[0],
            device_id={"mesh": partner}, device_id_type=MESH).wait_send()
    for way, size in enumerate(moved):
        if size:
            whole = down.at[pl.ds(0, size)]
            pltpu.make_async_remote_copy(
                src_ref=whole, dst_ref=whole, send_sem=w_send.at[way], recv_sem=w_recv.at[0],
                device_id={"member": twin}, device_id_type=MESH).wait_send()


def solution(mesh):
    ring, party = mesh.shape["mesh"], mesh.shape["member"]

    def on_device(node_states, projection, output_weight, up_weight, down_weight,
                  attention_gain, feedforward_gain, tile_lists, tile_counts):
        members, rows, width = node_states.shape
        tiles = tile_lists.shape[0]
        head = width // HEADS
        inner = up_weight.shape[1]
        hbm = pl.BlockSpec(memory_space=pltpu.HBM)
        bf16, f32 = jnp.bfloat16, jnp.float32
        copies = members * tiles * PIECES + LAST - 1
        keys = 3 * rows
        return pl.pallas_call(
            functools.partial(kernel, ring, party, tiles),
            out_shape=pltpu.VMEM(node_states.shape, bf16),
            in_specs=[hbm] * 9,
            out_specs=pl.BlockSpec(memory_space=pltpu.VMEM),
            scratch_shapes=[
                pltpu.VMEM((3, members, rows, width), bf16),
                pltpu.VMEM((members, rows, width), bf16),
                pltpu.VMEM((HEADS, width, 3 * head), bf16),
                pltpu.VMEM((width, width), bf16),
                pltpu.VMEM((width, inner), bf16),
                pltpu.VMEM((inner, width), bf16),
                pltpu.VMEM((members, HEADS, rows, head), bf16),
                pltpu.VMEM((members, HEADS, keys, head), bf16),
                pltpu.VMEM((members, HEADS, keys, 2 * head), bf16),
                pltpu.VMEM((members, HEADS, rows, 2 * head), f32),
                pltpu.VMEM((members, HEADS, rows, head), f32),
                pltpu.VMEM((members, HEADS, rows, head), bf16),
                pltpu.VMEM((members, rows, inner), bf16),
                pltpu.VMEM((members, rows, width), bf16),
                pltpu.VMEM((members, rows, width), bf16),
                pltpu.VMEM((members, rows, width), f32),
                pltpu.SMEM((tiles, 3 * tiles), f32),
                pltpu.VMEM((width,), f32),
                pltpu.VMEM((width,), f32),
                pltpu.SMEM(tile_lists.shape, jnp.int32),
                pltpu.SMEM(tile_counts.shape, jnp.int32),
                pltpu.SemaphoreType.DMA((7,)),
                pltpu.SemaphoreType.DMA,
                pltpu.SemaphoreType.DMA((copies,)),
                pltpu.SemaphoreType.DMA,
                pltpu.SemaphoreType.DMA((len(FAR),)),
                pltpu.SemaphoreType.DMA((5,)),
                pltpu.SemaphoreType.DMA((SLOTS,)),
            ],
            compiler_params=pltpu.CompilerParams(
                collective_id=0, has_side_effects=True, vmem_limit_bytes=60000000
            ),
        )(node_states, projection, output_weight, up_weight, down_weight,
          attention_gain, feedforward_gain, tile_lists, tile_counts)

    in_specs = (
        P("member", "mesh", None), P("member", None), P("member", None),
        P("member", None), P("member", None), P(), P(), P("mesh", None), P("mesh"),
    )
    return jax.shard_map(
        on_device, mesh=mesh, in_specs=in_specs,
        out_specs=P("member", "mesh", None), check_vma=False)
```
